32 devices in a mesh: owner: 8 (over z, core), sub: 4 (over y, x).
Axes of the slice: x: 2, y: 2, z: 4, core: 2. Of those that a mesh axis runs over, the one named last changes fastest.
Arguments:
- residual: float32 [256, 4608], P('owner', 'sub'), may hold values from -6 to 6
- counts: int32 [8, 16], P('owner', 'sub'), may hold values from 1 to 36
- assembly: int32 [8, 16, 36, 2304], P('owner', 'sub'), may hold values from 0 to 1, as said below
- level_two: float32 [8, 2304, 2304], P('owner', 'sub'), as said below
- block_inverse: float32 [8, 2304, 144], P('owner', 'sub'), as said below
Outputs:
- corrections: float32 [256, 4608], P('owner', 'sub')
- level_residual: float32 [8, 2304, 256], P('owner', 'sub')
The draws below stay inside these ranges and needn't reach their ends.
Inputs may be any that keep to these rules, and one draw needn't show every extreme that they name: `assembly`: every row of each [36, 2304] block holds exactly one 1; split the 2304 columns into 4 equal ranges and a group's positions into runs of 4: the 144 rows of one run (live or not) put at most 72 of their 1s into one range, and in every run some range gets exactly 72. `level_two`: each group's matrix is symmetric positive definite. `block_inverse`: each diagonal block is symmetric positive definite.
All inputs are finite; a program needn't handle non-finite values.
Results may differ from the reference program's by a relative error of at most 0.0003.
Values sent between devices are 32-bit elements; how exact they have to be, the bound alone decides.
No kernel may reach another device: no remote copies, remote signals or barrier semaphores. Data moves between devices by JAX's collectives and lax.ppermute only.
A program may use at most 64 MiB of HBM per device.

```python
import math
import jax
import jax.numpy as jnp
from jax import lax

PRIM = 36
NC = 2304
BLOCK = 144
ITERS = 4
SUB_DEV = 4
RHS = 256
GSUBS = 16
GROUPS = 8
SUBS = 128
ROUTE = 72
N_OWNER = 8
N_SUB = 4


def one_run(key):
    rows = SUB_DEV * PRIM
    held = NC // N_SUB
    key_a, key_b, key_c, key_d = jax.random.split(key, 4)
    first = jax.random.randint(key_a, (), 0, N_SUB).astype(jnp.int32)
    others = jax.random.permutation(key_b, (N_SUB - 1) * ROUTE).astype(jnp.int32)
    other_holder = others // ROUTE
    other_holder = other_holder + (other_holder >= first).astype(jnp.int32)
    holders = jnp.concatenate([jnp.zeros((ROUTE,), jnp.int32) + first, other_holder[:rows - ROUTE]])
    holders = jax.random.permutation(key_c, holders)
    offsets = jax.random.randint(key_d, (rows,), 0, held).astype(jnp.int32)
    return holders * held + offsets


def draw_assembly(key, part):
    keys = jax.random.split(jax.random.fold_in(key, 11), GROUPS * N_SUB)
    picks = jax.vmap(one_run)(keys).reshape(GROUPS, GSUBS, PRIM)
    columns = lax.broadcasted_iota(jnp.int32, (GROUPS, GSUBS, PRIM, NC), 3)
    return (columns == picks[..., None]).astype(jnp.int32)


def one_matrix(key):
    key_a, key_b, key_c = jax.random.split(key, 3)
    noise = jax.random.normal(key_a, (NC, NC), jnp.float32)
    eye = jnp.eye(NC, dtype=jnp.float32)
    off = (noise + noise.T) * (0.5 / math.sqrt(NC)) * (1.0 - eye)
    rowsum = jnp.sum(jnp.abs(off), axis=1)
    lift = jax.random.uniform(key_b, (NC,), jnp.float32, 0.05, 1.0) * jnp.mean(rowsum)
    diag = 1.25 * rowsum + lift
    matrix = (off + diag[:, None] * eye) / jnp.mean(diag)
    return matrix


def draw_level_two(key, part):
    keys = jax.random.split(jax.random.fold_in(key, 23), GROUPS)
    return lax.map(one_matrix, keys)


def draw_block_inverse(key, part):
    nblocks = NC // BLOCK
    key_a, key_b = jax.random.split(jax.random.fold_in(key, 37))
    noise = jax.random.uniform(key_a, (GROUPS, nblocks, BLOCK, BLOCK), jnp.float32, -1.0, 1.0)
    eye = jnp.eye(BLOCK, dtype=jnp.float32)
    off = (noise + jnp.swapaxes(noise, 2, 3)) * (0.2 / BLOCK) * (1.0 - eye)
    diag = jnp.exp(jax.random.uniform(key_b, (GROUPS, nblocks, BLOCK), jnp.float32, -0.7, 0.7))
    blocks = off + diag[..., None] * eye
    return blocks.reshape(GROUPS, NC, BLOCK)


def with_ends(values, key, low, largest):
    extent = values.shape
    spot = [jax.random.randint(jax.random.fold_in(key, axis), (), 0, extent[axis]) for axis in range(len(extent))]
    values = values.at[tuple(spot)].set(low)
    longest = extent.index(max(extent))
    spot[longest] = (spot[longest] + 1) % extent[longest]
    return values.at[tuple(spot)].set(largest)


def block_scale(own_key, extent, cuts, smallest, largest):
    gain, own = 1.0, jax.random.fold_in(own_key, 6)
    for position, shards_of in cuts:
        steps = jnp.exp(jax.random.uniform(jax.random.fold_in(own, position), (shards_of,), jnp.float32, smallest / len(cuts), largest / len(cuts)))
        gain = gain * jnp.repeat(steps, extent[position] // shards_of).reshape([-1 if axis == position else 1 for axis in range(len(extent))])
    return gain


def gaussian(own_key, shape, width, most, shards=(), kind=jnp.bfloat16):
    array = width * jax.random.normal(own_key, shape, jnp.float32)
    if shards:
        array = array * block_scale(own_key, shape, shards, -0.22, 0.18)
    return jnp.clip(array, -most, most).astype(kind)


def setup_inputs(seed: int = 0) -> dict:
    key_list = jax.random.split(jax.random.key(seed), 6)
    return {
        "residual": gaussian(key_list[0], (RHS, SUBS * PRIM), 1.0, 6.0, ((0, 8), (1, 4)), jnp.float32),
        "counts": with_ends(jax.random.randint(key_list[1], (GROUPS, GSUBS), 1, PRIM + 1), jax.random.fold_in(key_list[1], 1), 1, PRIM).astype(jnp.int32),
        "assembly": draw_assembly(jax.random.fold_in(key_list[5], 71), 0),
        "level_two": draw_level_two(jax.random.fold_in(key_list[5], 71), 0),
        "block_inverse": draw_block_inverse(jax.random.fold_in(key_list[5], 71), 0),
    }


def precondition(inverse, vector):
    nblocks = NC // BLOCK
    blocks = inverse.reshape(nblocks, BLOCK, BLOCK)
    shaped = vector.reshape(nblocks, BLOCK, RHS)
    return jnp.einsum("bij,bjr->bir", blocks, shaped, precision=lax.Precision.HIGHEST).reshape(NC, RHS)


def solve_group(items):
    local, count_row, blocks, matrix, inverse = items
    live = (lax.broadcasted_iota(jnp.int32, (GSUBS, PRIM), 1) < count_row[:, None]).astype(jnp.float32)
    basis = blocks.reshape(GSUBS * PRIM, NC).astype(jnp.float32) * live.reshape(GSUBS * PRIM)[:, None]
    rhs = jnp.dot(basis.T, local, precision=lax.Precision.HIGHEST, preferred_element_type=jnp.float32)
    solution = jnp.zeros((NC, RHS), jnp.float32)
    resid = rhs
    zvec = precondition(inverse, resid)
    direction = zvec
    rz_now = jnp.sum(resid * zvec, axis=0)
    for step in range(ITERS):
        image = jnp.dot(matrix, direction, precision=lax.Precision.HIGHEST, preferred_element_type=jnp.float32)
        alpha = rz_now / jnp.sum(direction * image, axis=0)
        solution = solution + alpha * direction
        resid = resid - alpha * image
        zvec = precondition(inverse, resid)
        rz_next = jnp.sum(resid * zvec, axis=0)
        direction = zvec + (rz_next / rz_now) * direction
        rz_now = rz_next
    corr = jnp.dot(basis, solution, precision=lax.Precision.HIGHEST, preferred_element_type=jnp.float32)
    return corr, resid


def reference(residual, counts, assembly, level_two, block_inverse):
    shaped = residual.reshape(RHS, N_SUB, N_OWNER, SUB_DEV, PRIM)
    local = jnp.transpose(shaped, (2, 1, 3, 4, 0)).reshape(N_OWNER, GSUBS * PRIM, RHS)
    corr, resid = lax.map(solve_group, (local, counts, assembly, level_two, block_inverse))
    back = corr.reshape(N_OWNER, N_SUB, SUB_DEV, PRIM, RHS)
    corrections = jnp.transpose(back, (4, 1, 0, 2, 3)).reshape(RHS, SUBS * PRIM)
    return corrections, resid
```

```python
import jax
import jax.numpy as jnp
from jax import lax
from jax.sharding import PartitionSpec as P

ITERS = 4


def pack_pairs(first, second):
    row = lax.broadcasted_iota(jnp.int32, first.shape, first.ndim - 2)
    col = lax.broadcasted_iota(jnp.int32, first.shape, first.ndim - 1)
    body = jnp.where(row <= col, first, second)
    diag = jnp.sum(jnp.where(row == col, second, 0.0), axis=-2, keepdims=True)
    return jnp.concatenate([body, diag], axis=-2)


def unpack_pairs(packed):
    size = packed.shape[-1]
    body = packed[..., :size, :]
    diag = packed[..., size:, :]
    flip = jnp.swapaxes(body, -1, -2)
    row = lax.broadcasted_iota(jnp.int32, body.shape, body.ndim - 2)
    col = lax.broadcasted_iota(jnp.int32, body.shape, body.ndim - 1)
    first = jnp.where(row <= col, body, flip)
    second = jnp.where(row > col, body, jnp.where(row < col, flip, diag))
    return first, second


def shards(residual, counts, assembly, level_two, block_inverse):
    highest = lax.Precision.HIGHEST
    high = lax.Precision.HIGH
    rows = level_two.shape[1]
    half = rows // 2
    width = level_two.shape[2]
    block = block_inverse.shape[2]
    held = rows // block
    slots = assembly.shape[1]
    prim = assembly.shape[2]
    dofs = slots * prim
    nsub = lax.axis_size("sub")
    me = lax.axis_index("sub")

    def swap(value, dist):
        return lax.ppermute(value, "sub", [(i, i ^ dist) for i in range(nsub)])

    def weight(dist):
        return bin(dist).count("1")

    def exchange():
        own = [
            lax.dynamic_slice(matrix, (0, (me ^ c) * rows), (rows, rows)) for c in range(nsub)
        ]
        blocks = {}
        for c in range(nsub):
            blocks[(0, c)] = own[c]
        for d in range(1, nsub):
            for e in range(d + 1, nsub):
                if weight(d) < weight(e):
                    blocks[(d, e)] = swap(own[d ^ e], d)
                elif weight(e) < weight(d):
                    blocks[(d, e)] = jnp.transpose(swap(own[d ^ e], e))
                else:
                    top = swap(own[d ^ e][:half], d)
                    bottom = swap(own[d ^ e][:, half:], e)
                    blocks[(d, e)] = jnp.concatenate([top, jnp.transpose(bottom)], axis=0)
        diag_pack = jnp.concatenate(
            [own[0][:half, half:], pack_pairs(own[0][:half, :half], own[0][half:, half:])], axis=0
        )
        inv_pack = pack_pairs(inv_own[: held // 2], inv_own[held // 2 :])
        inverses = [inv_own]
        for d in range(1, nsub):
            got = swap(diag_pack, d)
            cross = got[:half]
            first, second = unpack_pairs(got[half:])
            blocks[(d, d)] = jnp.concatenate(
                [
                    jnp.concatenate([first, cross], axis=1),
                    jnp.concatenate([jnp.transpose(cross), second], axis=1),
                ],
                axis=0,
            )
            got = swap(inv_pack, d)
            inverses.append(jnp.concatenate(unpack_pairs(got), axis=0))
        full = jnp.concatenate(
            [
                jnp.concatenate(
                    [
                        blocks[(d, e)] if d <= e else jnp.transpose(blocks[(e, d)])
                        for e in range(nsub)
                    ],
                    axis=1,
                )
                for d in range(nsub)
            ],
            axis=0,
        )
        inverse = jnp.concatenate(inverses, axis=0)
        return full, inverse

    matrix = level_two[0]
    inv_own = block_inverse[0].reshape(held, block, block)
    paired = held % 2 == 0
    if paired:
        order = me
        full, inverse = exchange()
    else:
        order = 0
        full = lax.all_gather(matrix, "sub", axis=0, tiled=True)
        inverse = lax.all_gather(inv_own, "sub", axis=0, tiled=True)

    local = lax.all_to_all(residual, "owner", split_axis=1, concat_axis=0, tiled=True)
    cols = local.shape[0] // nsub
    flat = assembly[0].reshape(dofs, width)
    target = jnp.sum(flat * lax.broadcasted_iota(jnp.int32, (dofs, width), 1), axis=1)
    live = lax.broadcasted_iota(jnp.int32, (slots, prim), 1) < counts[0][:, None]
    target = jnp.where(live.reshape(dofs), target, -1).astype(jnp.float32)
    pieces = []
    for d in range(nsub):
        piece = lax.dynamic_slice(local, ((me ^ d) * cols, 0), (cols, dofs))
        piece = jnp.concatenate([piece, target[None]], axis=0)
        pieces.append(piece if d == 0 else swap(piece, d))
    every = jnp.concatenate(pieces, axis=1)
    mine = every[:cols]
    goal = every[cols].astype(jnp.int32)
    relative = jnp.where(goal < 0, -1, ((goal // rows) ^ order) * rows + goal % rows)
    basis = (
        relative[:, None] == lax.broadcasted_iota(jnp.int32, (nsub * dofs, width), 1)
    ).astype(jnp.float32)
    resid = jnp.dot(mine, basis, precision=highest, preferred_element_type=jnp.float32)

    def precond(vector):
        shaped = vector.reshape(cols, width // block, block)
        return jnp.einsum("rbi,bij->rbj", shaped, inverse, precision=high).reshape(cols, width)

    def row_sum(left, right):
        return jnp.sum(left * right, axis=1, keepdims=True)

    answer = jnp.zeros_like(resid)
    zvec = precond(resid)
    direction = zvec
    rz_now = row_sum(resid, zvec)
    for step in range(ITERS):
        image = jnp.dot(direction, full, precision=high, preferred_element_type=jnp.float32)
        alpha = rz_now / row_sum(direction, image)
        answer = answer + alpha * direction
        resid = resid - alpha * image
        if step + 1 < ITERS:
            zvec = precond(resid)
            rz_next = row_sum(resid, zvec)
            direction = zvec + rz_next / rz_now * direction
            rz_now = rz_next
    corr = lax.dot_general(
        answer, basis, (((1,), (1,)), ((), ())), precision=highest,
        preferred_element_type=jnp.float32,
    )

    def back(array, size, first):
        got = []
        for d in range(nsub):
            piece = lax.dynamic_slice(array, (0, (d ^ first) * size), (cols, size))
            got.append(piece if d == 0 else swap(piece, d))
        got = jnp.stack(got)
        return jnp.concatenate(
            [lax.dynamic_index_in_dim(got, me ^ c, 0, keepdims=False) for c in range(nsub)], axis=0
        )

    corrections = lax.all_to_all(
        back(corr, dofs, 0), "owner", split_axis=0, concat_axis=1, tiled=True
    )
    return (corrections, jnp.transpose(back(resid, rows, 0 if paired else me))[None])


def solution(mesh):
    in_specs = (
        P("owner", "sub"),
        P("owner", "sub"),
        P("owner", "sub", None, None),
        P("owner", "sub", None),
        P("owner", "sub", None),
    )
    out_specs = (P("owner", "sub"), P("owner", "sub", None))
    return jax.shard_map(shards, mesh=mesh, in_specs=in_specs, out_specs=out_specs, check_vma=False)
```

```python
import jax
import jax.numpy as jnp
from jax import lax
from jax.experimental import pallas as pl
from jax.experimental.pallas import tpu as pltpu
from jax.sharding import PartitionSpec as P

ITERS = 4


def pack_pairs(first, second):
    row = lax.broadcasted_iota(jnp.int32, first.shape, first.ndim - 2)
    col = lax.broadcasted_iota(jnp.int32, first.shape, first.ndim - 1)
    body = jnp.where(row <= col, first, second)
    diag = jnp.sum(jnp.where(row == col, second, 0.0), axis=-2, keepdims=True)
    return jnp.concatenate([body, diag], axis=-2)


def unpack_pairs(packed):
    size = packed.shape[-1]
    body = packed[..., :size, :]
    diag = packed[..., size:, :]
    flip = jnp.swapaxes(body, -1, -2)
    row = lax.broadcasted_iota(jnp.int32, body.shape, body.ndim - 2)
    col = lax.broadcasted_iota(jnp.int32, body.shape, body.ndim - 1)
    first = jnp.where(row <= col, body, flip)
    second = jnp.where(row > col, body, jnp.where(row < col, flip, diag))
    return first, second


LANE = 128


def halves(value):
    top = value.astype(jnp.bfloat16)
    return top, (value - top.astype(jnp.float32)).astype(jnp.bfloat16)


def solve(pieces, kinds, inv_hi, inv_lo, rhs, nsub, rows, half, cut):
    span = -(-rows // LANE) * LANE
    total = nsub * span
    cols = rhs.shape[0]
    rest = rows - cut
    rest_pad = -(-rest // LANE) * LANE
    half_pad = -(-half // LANE) * LANE
    tile = 2 * LANE
    count = len(pieces)
    f32 = jnp.float32

    def body(*refs):
        srcs = refs[: count + 2]
        rhs_ref = refs[count + 2]
        x_ref, r_ref = refs[count + 3 : count + 5]
        scratch = refs[count + 5 :]
        bufs = scratch[: count + 2]
        a_hi, a_lo, tmp, packed, slim, p_ref, s_ref, w_ref, sems = scratch[count + 2 :]
        p_hi, p_lo = bufs[count:]
        copies = [
            pltpu.make_async_copy(srcs[i], bufs[i], sems.at[i]) for i in range(count + 2)
        ]
        for copy in copies:
            copy.start()
        tmp[...] = jnp.zeros((span, span), f32)
        packed[...] = jnp.zeros((rest_pad, rest_pad), f32)
        slim[...] = jnp.zeros((span, half_pad), f32)

        def place(d, e):
            for k in range(span // LANE):
                strip = tmp[k * LANE : (k + 1) * LANE, :]
                hi, lo = halves(strip)
                at = (slice(d * span + k * LANE, d * span + (k + 1) * LANE), slice(e * span, (e + 1) * span))
                a_hi[at] = hi
                a_lo[at] = lo
                if d != e:
                    flipped = jnp.transpose(strip)
                    hi, lo = halves(flipped)
                    at = (slice(e * span, (e + 1) * span), slice(d * span + k * LANE, d * span + (k + 1) * LANE))
                    a_hi[at] = hi
                    a_lo[at] = lo

        for i, (kind, d, e) in enumerate(kinds):
            copies[i].wait()
            buf = bufs[i]
            if kind == "block":
                tmp[:rows, :rows] = buf[...]
                place(d, e)
            elif kind == "turned":
                tmp[:rows, :rows] = buf[...]
                place(e, d)
            elif kind == "top":
                tmp[:half, :rows] = buf[...]
            elif kind == "bottom":
                slim[:rows, : rows - half] = buf[...]
                turned = jnp.transpose(slim[...])
                tmp[half:rows, :rows] = turned[: rows - half, :rows]
                place(d, e)
            else:
                packed[:rest, :rest] = buf[cut:rows, :]
                mix = packed[...]
                flip = jnp.transpose(mix)
                row = lax.broadcasted_iota(jnp.int32, (rest_pad, rest_pad), 0)
                col = lax.broadcasted_iota(jnp.int32, (rest_pad, rest_pad), 1)
                first = jnp.where(row <= col, mix, flip)
                second = jnp.where(row > col, mix, flip)[:rest, :rest]
                onto = (row == col)[:rest, :rest]
                second = jnp.where(onto, buf[rows : rows + 1, :], second)
                tmp[:cut, :cut] = first[:cut, :cut]
                cross = buf[:cut, :]
                tmp[:cut, cut:rows] = cross
                packed[:cut, :rest] = cross
                tmp[cut:rows, :cut] = jnp.transpose(packed[:cut, :])[:rest, :]
                tmp[cut:rows, cut:rows] = second
                place(d, d)
        copies[count].wait()
        copies[count + 1].wait()

        def split_into(value):
            hi, lo = halves(value)
            s_ref[:cols, :] = hi
            s_ref[cols:, :] = lo

        def product(left, right_hi, right_lo):
            both = jnp.dot(left, right_hi, preferred_element_type=f32)
            low = jnp.dot(left[:cols], right_lo, preferred_element_type=f32)
            return both[:cols] + (both[cols:] + low)

        def times_matrix():
            def one(n, carry):
                at = pl.ds(pl.multiple_of(n * tile, tile), tile)
                w_ref[:, at] = product(s_ref[...], a_hi[:, at], a_lo[:, at])
                return carry

            lax.fori_loop(0, total // tile, one, 0)

        def precond(value):
            split_into(value)

            def one(n, carry):
                at = pl.ds(pl.multiple_of(n * span, LANE), span)
                w_ref[:, at] = product(s_ref[:, at], p_hi[at, :], p_lo[at, :])
                return carry

            lax.fori_loop(0, nsub, one, 0)
            return w_ref[...]

        def row_sum(left, right):
            return jnp.sum(left * right, axis=1, keepdims=True)

        r_ref[...] = rhs_ref[...]
        x_ref[...] = jnp.zeros((cols, total), f32)
        p_ref[...] = precond(rhs_ref[...])
        rz_now = row_sum(r_ref[...], p_ref[...])
        for step in range(ITERS):
            split_into(p_ref[...])
            times_matrix()
            alpha = rz_now / row_sum(p_ref[...], w_ref[...])
            x_ref[...] = x_ref[...] + alpha * p_ref[...]
            r_ref[...] = r_ref[...] - alpha * w_ref[...]
            if step + 1 < ITERS:
                zvec = precond(r_ref[...])
                rz_next = row_sum(r_ref[...], zvec)
                p_ref[...] = zvec + rz_next / rz_now * p_ref[...]
                rz_now = rz_next

    anywhere = pl.BlockSpec(memory_space=pl.ANY)
    near = pl.BlockSpec(memory_space=pltpu.VMEM)
    out = jax.ShapeDtypeStruct((cols, total), f32)
    return pl.pallas_call(
        body,
        out_shape=(out, out),
        in_specs=[anywhere] * (count + 2) + [near],
        out_specs=(near, near),
        scratch_shapes=[pltpu.VMEM(v.shape, v.dtype) for v in (*pieces, inv_hi, inv_lo)]
        + [
            pltpu.VMEM((total, total), jnp.bfloat16),
            pltpu.VMEM((total, total), jnp.bfloat16),
            pltpu.VMEM((span, span), f32),
            pltpu.VMEM((rest_pad, rest_pad), f32),
            pltpu.VMEM((span, half_pad), f32),
            pltpu.VMEM((cols, total), f32),
            pltpu.VMEM((2 * cols, total), jnp.bfloat16),
            pltpu.VMEM((cols, total), f32),
            pltpu.SemaphoreType.DMA((count + 2,)),
        ],
        compiler_params=pltpu.CompilerParams(vmem_limit_bytes=62 * 1024 * 1024),
    )(*pieces, inv_hi, inv_lo, rhs)


def shards(residual, counts, assembly, level_two, block_inverse):
    highest = lax.Precision.HIGHEST
    high = lax.Precision.HIGH
    rows = level_two.shape[1]
    half = rows // 2
    width = level_two.shape[2]
    block = block_inverse.shape[2]
    held = rows // block
    slots = assembly.shape[1]
    prim = assembly.shape[2]
    dofs = slots * prim
    nsub = lax.axis_size("sub")
    me = lax.axis_index("sub")

    def swap(value, dist):
        return lax.ppermute(value, "sub", [(i, i ^ dist) for i in range(nsub)])

    def weight(dist):
        return bin(dist).count("1")

    def exchange():
        own = [
            lax.dynamic_slice(matrix, (0, (me ^ c) * rows), (rows, rows)) for c in range(nsub)
        ]
        cut = max(half // LANE * LANE, 0)
        rest = rows - cut
        first = jnp.pad(own[0][:cut, :cut], ((0, rest - cut), (0, rest - cut)))
        diag_pack = jnp.concatenate([own[0][:cut, cut:], pack_pairs(first, own[0][cut:, cut:])], axis=0)
        inv_pack = pack_pairs(inv_own[: held // 2], inv_own[held // 2 :])
        inverses = [inv_own]
        for d in range(1, nsub):
            inverses.append(jnp.concatenate(unpack_pairs(swap(inv_pack, d)), axis=0))
        pieces, kinds = [], []

        def add(value, kind, d, e):
            pieces.append(value)
            kinds.append((kind, d, e))

        for c in range(nsub):
            add(own[c], "block", 0, c)
        for d in range(1, nsub):
            add(swap(diag_pack, d), "diag", d, d)
        for d in range(1, nsub):
            for e in range(d + 1, nsub):
                if weight(d) < weight(e):
                    add(swap(own[d ^ e], d), "block", d, e)
                elif weight(e) < weight(d):
                    add(swap(own[d ^ e], e), "turned", d, e)
        for d in range(1, nsub):
            for e in range(d + 1, nsub):
                if weight(d) == weight(e):
                    add(swap(own[d ^ e][:half], d), "top", d, e)
                    add(swap(own[d ^ e][:, half:], e), "bottom", d, e)
        inverse = jnp.concatenate(inverses, axis=0).reshape(nsub, rows, block)
        wide = jnp.concatenate([inverse] * held, axis=2)
        row = lax.broadcasted_iota(jnp.int32, wide.shape, 1) // block
        col = lax.broadcasted_iota(jnp.int32, wide.shape, 2) // block
        wide = jnp.where(row == col, wide, 0.0)
        wide = jnp.pad(wide, ((0, 0), (0, span - rows), (0, span - rows))).reshape(nsub * span, span)
        top = lax.reduce_precision(wide, 8, 7)
        return pieces, kinds, top.astype(jnp.bfloat16), (wide - top).astype(jnp.bfloat16), cut

    matrix = level_two[0]
    inv_own = block_inverse[0].reshape(held, block, block)
    paired = held % 2 == 0
    if paired:
        order = me
        span = -(-rows // LANE) * LANE
        pieces, kinds, inv_hi, inv_lo, cut = exchange()
    else:
        order = 0
        span = rows
        full = lax.all_gather(matrix, "sub", axis=0, tiled=True)
        inverse = lax.all_gather(inv_own, "sub", axis=0, tiled=True)

    local = lax.all_to_all(residual, "owner", split_axis=1, concat_axis=0, tiled=True)
    cols = local.shape[0] // nsub
    flat = assembly[0].reshape(dofs, width)
    target = jnp.sum(flat * lax.broadcasted_iota(jnp.int32, (dofs, width), 1), axis=1)
    live = lax.broadcasted_iota(jnp.int32, (slots, prim), 1) < counts[0][:, None]
    target = jnp.where(live.reshape(dofs), target, -1).astype(jnp.float32)
    columns = []
    for d in range(nsub):
        piece = lax.dynamic_slice(local, ((me ^ d) * cols, 0), (cols, dofs))
        piece = jnp.concatenate([piece, target[None]], axis=0)
        columns.append(piece if d == 0 else swap(piece, d))
    every = jnp.concatenate(columns, axis=1)
    mine = every[:cols]
    goal = every[cols].astype(jnp.int32)
    relative = jnp.where(goal < 0, -1, ((goal // rows) ^ order) * span + goal % rows)
    basis = (
        relative[:, None] == lax.broadcasted_iota(jnp.int32, (nsub * dofs, nsub * span), 1)
    ).astype(jnp.float32)
    resid = jnp.dot(mine, basis, precision=highest, preferred_element_type=jnp.float32)

    def precond(vector):
        shaped = vector.reshape(cols, width // block, block)
        return jnp.einsum("rbi,bij->rbj", shaped, inverse, precision=high).reshape(cols, width)

    def row_sum(left, right):
        return jnp.sum(left * right, axis=1, keepdims=True)

    if paired:
        answer, resid = solve(pieces, kinds, inv_hi, inv_lo, resid, nsub, rows, half, cut)
    else:
        answer = jnp.zeros_like(resid)
        zvec = precond(resid)
        direction = zvec
        rz_now = row_sum(resid, zvec)
        for step in range(ITERS):
            image = jnp.dot(direction, full, precision=high, preferred_element_type=jnp.float32)
            alpha = rz_now / row_sum(direction, image)
            answer = answer + alpha * direction
            resid = resid - alpha * image
            if step + 1 < ITERS:
                zvec = precond(resid)
                rz_next = row_sum(resid, zvec)
                direction = zvec + rz_next / rz_now * direction
                rz_now = rz_next
    corr = lax.dot_general(
        answer, basis, (((1,), (1,)), ((), ())), precision=highest,
        preferred_element_type=jnp.float32,
    )

    def back(array, size, step, first):
        got = []
        for d in range(nsub):
            piece = lax.dynamic_slice(array, (0, (d ^ first) * step), (cols, size))
            got.append(piece if d == 0 else swap(piece, d))
        got = jnp.stack(got)
        return jnp.concatenate(
            [lax.dynamic_index_in_dim(got, me ^ c, 0, keepdims=False) for c in range(nsub)], axis=0
        )

    corrections = lax.all_to_all(
        back(corr, dofs, dofs, 0), "owner", split_axis=0, concat_axis=1, tiled=True
    )
    return (corrections, jnp.transpose(back(resid, rows, span, 0 if paired else me))[None])


def solution(mesh):
    in_specs = (
        P("owner", "sub"),
        P("owner", "sub"),
        P("owner", "sub", None, None),
        P("owner", "sub", None),
        P("owner", "sub", None),
    )
    out_specs = (P("owner", "sub"), P("owner", "sub", None))
    return jax.shard_map(shards, mesh=mesh, in_specs=in_specs, out_specs=out_specs, check_vma=False)
```

```python
import jax
import jax.numpy as jnp
from jax import lax
from jax.experimental import pallas as pl
from jax.experimental.layout import Layout, with_layout_constraint
from jax.experimental.pallas import tpu as pltpu
from jax.sharding import PartitionSpec as P

ITERS = 4


def pack_pairs(first, second):
    row = lax.broadcasted_iota(jnp.int32, first.shape, first.ndim - 2)
    col = lax.broadcasted_iota(jnp.int32, first.shape, first.ndim - 1)
    body = jnp.where(row <= col, first, second)
    diag = jnp.sum(jnp.where(row == col, second, 0.0), axis=-2, keepdims=True)
    return jnp.concatenate([body, diag], axis=-2)


def unpack_pairs(packed):
    size = packed.shape[-1]
    body = packed[..., :size, :]
    diag = packed[..., size:, :]
    flip = jnp.swapaxes(body, -1, -2)
    row = lax.broadcasted_iota(jnp.int32, body.shape, body.ndim - 2)
    col = lax.broadcasted_iota(jnp.int32, body.shape, body.ndim - 1)
    first = jnp.where(row <= col, body, flip)
    second = jnp.where(row > col, body, jnp.where(row < col, flip, diag))
    return first, second


LANE = 128


def halves(value):
    top = value.astype(jnp.bfloat16)
    return top, (value - top.astype(jnp.float32)).astype(jnp.bfloat16)


def solve(pieces, kinds, inv_hi, inv_lo, rhs, nsub, rows, half, cut):
    span = -(-rows // LANE) * LANE
    total = nsub * span
    cols = rhs.shape[0]
    rest = rows - cut
    rest_pad = -(-rest // LANE) * LANE
    tile = 2 * LANE
    count = len(pieces)
    f32 = jnp.float32

    def body(*refs):
        srcs = refs[: count + 2]
        rhs_ref = refs[count + 2]
        x_ref, r_ref = refs[count + 3 : count + 5]
        scratch = refs[count + 5 :]
        bufs = scratch[: count + 2]
        a_hi, a_lo, tmp, packed, p_ref, s_ref, w_ref, sems = scratch[count + 2 :]
        p_hi, p_lo = bufs[count:]
        copies = [
            pltpu.make_async_copy(srcs[i], bufs[i], sems.at[i]) for i in range(count + 2)
        ]
        for copy in copies:
            copy.start()
        tmp[...] = jnp.zeros((span, span), f32)
        packed[...] = jnp.zeros((rest_pad, rest_pad), f32)

        def place(d, e):
            for k in range(span // LANE):
                strip = tmp[k * LANE : (k + 1) * LANE, :]
                hi, lo = halves(strip)
                at = (slice(d * span + k * LANE, d * span + (k + 1) * LANE), slice(e * span, (e + 1) * span))
                a_hi[at] = hi
                a_lo[at] = lo
                if d != e:
                    flipped = jnp.transpose(strip)
                    hi, lo = halves(flipped)
                    at = (slice(e * span, (e + 1) * span), slice(d * span + k * LANE, d * span + (k + 1) * LANE))
                    a_hi[at] = hi
                    a_lo[at] = lo

        for i, (kind, d, e) in enumerate(kinds):
            copies[i].wait()
            buf = bufs[i]
            if kind == "block":
                tmp[:rows, :rows] = buf[...]
                place(d, e)
            elif kind == "turned":
                tmp[:rows, :rows] = buf[...]
                place(e, d)
            elif kind == "top":
                tmp[:half, :rows] = buf[...]
            elif kind == "bottom":
                tmp[half:rows, :rows] = buf[...]
                place(d, e)
            else:
                packed[:rest, :rest] = buf[:, cut:rows]
                mix = packed[...]
                flip = jnp.transpose(mix)
                row = lax.broadcasted_iota(jnp.int32, (rest_pad, rest_pad), 0)
                col = lax.broadcasted_iota(jnp.int32, (rest_pad, rest_pad), 1)
                first = jnp.where(row <= col, mix, flip)
                second = jnp.where(row > col, mix, flip)[:rest, :rest]
                onto = (row == col)[:rest, :rest]
                second = jnp.where(onto, buf[:, rows : rows + 1], second)
                tmp[:cut, :cut] = first[:cut, :cut]
                cross = buf[:, :cut]
                tmp[cut:rows, :cut] = cross
                packed[:rest, :cut] = cross
                tmp[:cut, cut:rows] = jnp.transpose(packed[:, :cut])[:, :rest]
                tmp[cut:rows, cut:rows] = second
                place(d, d)
        copies[count].wait()
        copies[count + 1].wait()

        def split_into(value):
            hi, lo = halves(value)
            s_ref[:cols, :] = hi
            s_ref[cols:, :] = lo

        def product(left, right_hi, right_lo):
            both = jnp.dot(left, right_hi, preferred_element_type=f32)
            low = jnp.dot(left[:cols], right_lo, preferred_element_type=f32)
            return both[:cols] + (both[cols:] + low)

        def times_matrix():
            def one(n, carry):
                at = pl.ds(pl.multiple_of(n * tile, tile), tile)
                w_ref[:, at] = product(s_ref[...], a_hi[:, at], a_lo[:, at])
                return carry

            lax.fori_loop(0, total // tile, one, 0)

        def precond(value):
            split_into(value)

            def one(n, carry):
                at = pl.ds(pl.multiple_of(n * span, LANE), span)
                w_ref[:, at] = product(s_ref[:, at], p_hi[at, :], p_lo[at, :])
                return carry

            lax.fori_loop(0, nsub, one, 0)
            return w_ref[...]

        def row_sum(left, right):
            return jnp.sum(left * right, axis=1, keepdims=True)

        r_ref[...] = rhs_ref[...]
        x_ref[...] = jnp.zeros((cols, total), f32)
        p_ref[...] = precond(rhs_ref[...])
        rz_now = row_sum(r_ref[...], p_ref[...])
        for step in range(ITERS):
            split_into(p_ref[...])
            times_matrix()
            alpha = rz_now / row_sum(p_ref[...], w_ref[...])
            x_ref[...] = x_ref[...] + alpha * p_ref[...]
            r_ref[...] = r_ref[...] - alpha * w_ref[...]
            if step + 1 < ITERS:
                zvec = precond(r_ref[...])
                rz_next = row_sum(r_ref[...], zvec)
                p_ref[...] = zvec + rz_next / rz_now * p_ref[...]
                rz_now = rz_next

    anywhere = pl.BlockSpec(memory_space=pl.ANY)
    near = pl.BlockSpec(memory_space=pltpu.VMEM)
    out = jax.ShapeDtypeStruct((cols, total), f32)
    return pl.pallas_call(
        body,
        out_shape=(out, out),
        in_specs=[anywhere] * (count + 2) + [near],
        out_specs=(near, near),
        scratch_shapes=[pltpu.VMEM(v.shape, v.dtype) for v in (*pieces, inv_hi, inv_lo)]
        + [
            pltpu.VMEM((total, total), jnp.bfloat16),
            pltpu.VMEM((total, total), jnp.bfloat16),
            pltpu.VMEM((span, span), f32),
            pltpu.VMEM((rest_pad, rest_pad), f32),
            pltpu.VMEM((cols, total), f32),
            pltpu.VMEM((2 * cols, total), jnp.bfloat16),
            pltpu.VMEM((cols, total), f32),
            pltpu.SemaphoreType.DMA((count + 2,)),
        ],
        compiler_params=pltpu.CompilerParams(vmem_limit_bytes=62 * 1024 * 1024),
    )(*pieces, inv_hi, inv_lo, rhs)


def shards(residual, counts, assembly, level_two, block_inverse):
    highest = lax.Precision.HIGHEST
    high = lax.Precision.HIGH
    rows = level_two.shape[1]
    half = rows // 2
    width = level_two.shape[2]
    block = block_inverse.shape[2]
    held = rows // block
    slots = assembly.shape[1]
    prim = assembly.shape[2]
    dofs = slots * prim
    nsub = lax.axis_size("sub")
    me = lax.axis_index("sub")

    def swap(value, dist):
        return lax.ppermute(value, "sub", [(i, i ^ dist) for i in range(nsub)])

    def weight(dist):
        return bin(dist).count("1")

    matrix = level_two[0]
    inv_own = block_inverse[0].reshape(held, block, block)
    paired = held % 2 == 0

    def own(value, c):
        return lax.dynamic_slice(value, (0, (me ^ c) * rows), (rows, rows))

    def plain(value):
        return with_layout_constraint(value, Layout(major_to_minor=tuple(range(value.ndim))))

    pairs = [(d, e) for d in range(1, nsub) for e in range(d + 1, nsub)]
    if paired:
        order = me
        span = -(-rows // LANE) * LANE
        early, moved, where = [], [], []
        for d, e in pairs:
            if weight(d) < weight(e):
                where.append(("block", d, e, d))
            elif weight(e) < weight(d):
                where.append(("turned", d, e, e))
        for kind, d, e, dist in where:
            early.append(plain(own(matrix, d ^ e)))
        early = list(lax.optimization_barrier(tuple(early)))
        for (kind, d, e, dist), value in zip(where, early):
            moved.append((swap(value, dist), kind, d, e))
        matrix, inv_own, residual, assembly, *early = lax.optimization_barrier(
            (matrix, inv_own, residual, assembly, *early)
        )
        inv_pack = pack_pairs(inv_own[: held // 2], inv_own[held // 2 :])
        inverses = [inv_own]
        for d in range(1, nsub):
            inverses.append(jnp.concatenate(unpack_pairs(swap(inv_pack, d)), axis=0))
    else:
        order = 0
        span = rows
        full = lax.all_gather(matrix, "sub", axis=0, tiled=True)
        inverse = lax.all_gather(inv_own, "sub", axis=0, tiled=True)

    local = lax.all_to_all(residual, "owner", split_axis=1, concat_axis=0, tiled=True)
    cols = local.shape[0] // nsub
    flat = assembly[0].reshape(dofs, width)
    target = jnp.sum(flat * lax.broadcasted_iota(jnp.int32, (dofs, width), 1), axis=1)
    live = lax.broadcasted_iota(jnp.int32, (slots, prim), 1) < counts[0][:, None]
    target = jnp.where(live.reshape(dofs), target, -1).astype(jnp.float32)
    sends = []
    for d in range(nsub):
        piece = lax.dynamic_slice(local, ((me ^ d) * cols, 0), (cols, dofs))
        piece = jnp.concatenate([piece, target[None]], axis=0)
        sends.append(piece)
    if paired:
        matrix, *sends = lax.optimization_barrier((matrix, *sends))
    columns = [value if d == 0 else swap(value, d) for d, value in enumerate(sends)]
    if paired:
        pieces, kinds = [], []

        def add(value, kind, d, e):
            pieces.append(value)
            kinds.append((kind, d, e))

        cut = half // LANE * LANE
        rest = rows - cut
        here = own(matrix, 0)
        first = jnp.pad(here[:cut, :cut], ((0, rest - cut), (0, rest - cut)))
        mixed = pack_pairs(first, here[cut:, cut:])
        diag_pack = plain(
            jnp.concatenate(
                [here[cut:, :cut], mixed[:rest], jnp.transpose(mixed[rest:])], axis=1
            )
        )
        add(here, "block", 0, 0)
        for c in range(1, nsub):
            kept = [v for v, (_, d, e, _) in zip(early, where) if d ^ e == c]
            add(kept[0] if kept else plain(own(matrix, c)), "block", 0, c)
        for item in moved:
            add(*item)
        for d in range(1, nsub):
            add(plain(swap(diag_pack, d)), "diag", d, d)
        for d, e in pairs:
            if weight(d) == weight(e):
                both = own(matrix, d ^ e)
                add(plain(swap(plain(both[:half]), d)), "top", d, e)
                add(plain(swap(plain(jnp.transpose(both[:, half:])), e)), "bottom", d, e)
        inverse = jnp.concatenate(inverses, axis=0).reshape(nsub, rows, block)
        wide = jnp.concatenate([inverse] * held, axis=2)
        row = lax.broadcasted_iota(jnp.int32, wide.shape, 1) // block
        col = lax.broadcasted_iota(jnp.int32, wide.shape, 2) // block
        wide = jnp.where(row == col, wide, 0.0)
        wide = jnp.pad(wide, ((0, 0), (0, span - rows), (0, span - rows))).reshape(nsub * span, span)
        top = lax.reduce_precision(wide, 8, 7)
        inv_hi, inv_lo = top.astype(jnp.bfloat16), (wide - top).astype(jnp.bfloat16)
    every = jnp.concatenate(columns, axis=1)
    mine = every[:cols]
    goal = every[cols].astype(jnp.int32)
    relative = jnp.where(goal < 0, -1, ((goal // rows) ^ order) * span + goal % rows)
    basis = (
        relative[:, None] == lax.broadcasted_iota(jnp.int32, (nsub * dofs, nsub * span), 1)
    ).astype(jnp.float32)
    resid = jnp.dot(mine, basis, precision=highest, preferred_element_type=jnp.float32)

    def precond(vector):
        shaped = vector.reshape(cols, width // block, block)
        return jnp.einsum("rbi,bij->rbj", shaped, inverse, precision=high).reshape(cols, width)

    def row_sum(left, right):
        return jnp.sum(left * right, axis=1, keepdims=True)

    if paired:
        answer, resid = solve(pieces, kinds, inv_hi, inv_lo, resid, nsub, rows, half, cut)
    else:
        answer = jnp.zeros_like(resid)
        zvec = precond(resid)
        direction = zvec
        rz_now = row_sum(resid, zvec)
        for step in range(ITERS):
            image = jnp.dot(direction, full, precision=high, preferred_element_type=jnp.float32)
            alpha = rz_now / row_sum(direction, image)
            answer = answer + alpha * direction
            resid = resid - alpha * image
            if step + 1 < ITERS:
                zvec = precond(resid)
                rz_next = row_sum(resid, zvec)
                direction = zvec + rz_next / rz_now * direction
                rz_now = rz_next
    corr = lax.dot_general(
        answer, basis, (((1,), (1,)), ((), ())), precision=high,
        preferred_element_type=jnp.float32,
    )

    def back(array, size, step, first):
        got = []
        for d in range(nsub):
            piece = lax.dynamic_slice(array, (0, (d ^ first) * step), (cols, size))
            got.append(piece if d == 0 else swap(piece, d))
        got = jnp.stack(got)
        return jnp.concatenate(
            [lax.dynamic_index_in_dim(got, me ^ c, 0, keepdims=False) for c in range(nsub)], axis=0
        )

    level_residual = back(resid, rows, span, 0 if paired else me)
    corrections = lax.all_to_all(
        back(corr, dofs, dofs, 0), "owner", split_axis=0, concat_axis=1, tiled=True
    )
    return (corrections, jnp.transpose(level_residual)[None])


def solution(mesh):
    in_specs = (
        P("owner", "sub"),
        P("owner", "sub"),
        P("owner", "sub", None, None),
        P("owner", "sub", None),
        P("owner", "sub", None),
    )
    out_specs = (P("owner", "sub"), P("owner", "sub", None))
    return jax.shard_map(shards, mesh=mesh, in_specs=in_specs, out_specs=out_specs, check_vma=False)
```

```python
import jax
import jax.numpy as jnp
from jax import lax
from jax.experimental import pallas as pl
from jax.experimental.layout import Layout, with_layout_constraint
from jax.experimental.pallas import tpu as pltpu
from jax.sharding import PartitionSpec as P

ITERS = 4


def pack_pairs(first, second):
    row = lax.broadcasted_iota(jnp.int32, first.shape, first.ndim - 2)
    col = lax.broadcasted_iota(jnp.int32, first.shape, first.ndim - 1)
    body = jnp.where(row <= col, first, second)
    diag = jnp.sum(jnp.where(row == col, second, 0.0), axis=-2, keepdims=True)
    return jnp.concatenate([body, diag], axis=-2)


def unpack_pairs(packed):
    size = packed.shape[-1]
    body = packed[..., :size, :]
    diag = packed[..., size:, :]
    flip = jnp.swapaxes(body, -1, -2)
    row = lax.broadcasted_iota(jnp.int32, body.shape, body.ndim - 2)
    col = lax.broadcasted_iota(jnp.int32, body.shape, body.ndim - 1)
    first = jnp.where(row <= col, body, flip)
    second = jnp.where(row > col, body, jnp.where(row < col, flip, diag))
    return first, second


LANE = 128


def halves(value):
    top = value.astype(jnp.bfloat16)
    return top, (value - top.astype(jnp.float32)).astype(jnp.bfloat16)


def solve(pieces, kinds, inv_hi, inv_lo, rhs, nsub, rows, half, cut):
    span = -(-rows // LANE) * LANE
    total = nsub * span
    cols = rhs.shape[0]
    rest = rows - cut
    rest_pad = -(-rest // LANE) * LANE
    tile = 2 * LANE
    count = len(pieces)
    f32 = jnp.float32

    def body(*refs):
        srcs = refs[: count + 2]
        rhs_ref = refs[count + 2]
        x_ref, r_ref = refs[count + 3 : count + 5]
        scratch = refs[count + 5 :]
        bufs = scratch[: count + 2]
        a_hi, a_lo, tmp, packed, p_ref, s_ref, w_ref, sems = scratch[count + 2 :]
        p_hi, p_lo = bufs[count:]
        copies = [
            pltpu.make_async_copy(srcs[i], bufs[i], sems.at[i]) for i in range(count + 2)
        ]
        for copy in copies:
            copy.start()
        tmp[...] = jnp.zeros((span, span), f32)
        packed[...] = jnp.zeros((rest_pad, rest_pad), f32)

        def place(d, e):
            for k in range(span // LANE):
                strip = tmp[k * LANE : (k + 1) * LANE, :]
                hi, lo = halves(strip)
                at = (slice(d * span + k * LANE, d * span + (k + 1) * LANE), slice(e * span, (e + 1) * span))
                a_hi[at] = hi
                a_lo[at] = lo
                if d != e:
                    flipped = jnp.transpose(strip)
                    hi, lo = halves(flipped)
                    at = (slice(e * span, (e + 1) * span), slice(d * span + k * LANE, d * span + (k + 1) * LANE))
                    a_hi[at] = hi
                    a_lo[at] = lo

        for i, (kind, d, e) in enumerate(kinds):
            copies[i].wait()
            buf = bufs[i]
            if kind == "block":
                tmp[:rows, :rows] = buf[...]
                place(d, e)
            elif kind == "turned":
                tmp[:rows, :rows] = buf[...]
                place(e, d)
            elif kind == "top":
                tmp[:half, :rows] = buf[...]
            elif kind == "bottom":
                tmp[half:rows, :rows] = buf[...]
                place(d, e)
            else:
                packed[:rest, :rest] = buf[:, cut:rows]
                mix = packed[...]
                flip = jnp.transpose(mix)
                row = lax.broadcasted_iota(jnp.int32, (rest_pad, rest_pad), 0)
                col = lax.broadcasted_iota(jnp.int32, (rest_pad, rest_pad), 1)
                first = jnp.where(row <= col, mix, flip)
                second = jnp.where(row > col, mix, flip)[:rest, :rest]
                onto = (row == col)[:rest, :rest]
                second = jnp.where(onto, buf[:, rows : rows + 1], second)
                tmp[:cut, :cut] = first[:cut, :cut]
                cross = buf[:, :cut]
                tmp[cut:rows, :cut] = cross
                packed[:rest, :cut] = cross
                tmp[:cut, cut:rows] = jnp.transpose(packed[:, :cut])[:, :rest]
                tmp[cut:rows, cut:rows] = second
                place(d, d)
        copies[count].wait()
        copies[count + 1].wait()

        def split_into(value):
            hi, lo = halves(value)
            s_ref[:cols, :] = hi
            s_ref[cols:, :] = lo

        def product(left, right_hi, right_lo):
            both = jnp.dot(left, right_hi, preferred_element_type=f32)
            low = jnp.dot(left[:cols], right_lo, preferred_element_type=f32)
            return both[:cols] + (both[cols:] + low)

        def times_matrix():
            def one(n, carry):
                at = pl.ds(pl.multiple_of(n * tile, tile), tile)
                w_ref[:, at] = product(s_ref[...], a_hi[:, at], a_lo[:, at])
                return carry

            lax.fori_loop(0, total // tile, one, 0)

        def precond(value):
            split_into(value)

            def one(n, carry):
                at = pl.ds(pl.multiple_of(n * span, LANE), span)
                w_ref[:, at] = product(s_ref[:, at], p_hi[at, :], p_lo[at, :])
                return carry

            lax.fori_loop(0, nsub, one, 0)
            return w_ref[...]

        def row_sum(left, right):
            return jnp.sum(left * right, axis=1, keepdims=True)

        r_ref[...] = rhs_ref[...]
        x_ref[...] = jnp.zeros((cols, total), f32)
        p_ref[...] = precond(rhs_ref[...])
        rz_now = row_sum(r_ref[...], p_ref[...])
        for step in range(ITERS):
            split_into(p_ref[...])
            times_matrix()
            alpha = rz_now / row_sum(p_ref[...], w_ref[...])
            x_ref[...] = x_ref[...] + alpha * p_ref[...]
            r_ref[...] = r_ref[...] - alpha * w_ref[...]
            if step + 1 < ITERS:
                zvec = precond(r_ref[...])
                rz_next = row_sum(r_ref[...], zvec)
                p_ref[...] = zvec + rz_next / rz_now * p_ref[...]
                rz_now = rz_next

    anywhere = pl.BlockSpec(memory_space=pl.ANY)
    near = pl.BlockSpec(memory_space=pltpu.VMEM)
    out = jax.ShapeDtypeStruct((cols, total), f32)
    return pl.pallas_call(
        body,
        out_shape=(out, out),
        in_specs=[anywhere] * (count + 2) + [near],
        out_specs=(near, near),
        scratch_shapes=[pltpu.VMEM(v.shape, v.dtype) for v in (*pieces, inv_hi, inv_lo)]
        + [
            pltpu.VMEM((total, total), jnp.bfloat16),
            pltpu.VMEM((total, total), jnp.bfloat16),
            pltpu.VMEM((span, span), f32),
            pltpu.VMEM((rest_pad, rest_pad), f32),
            pltpu.VMEM((cols, total), f32),
            pltpu.VMEM((2 * cols, total), jnp.bfloat16),
            pltpu.VMEM((cols, total), f32),
            pltpu.SemaphoreType.DMA((count + 2,)),
        ],
        compiler_params=pltpu.CompilerParams(vmem_limit_bytes=62 * 1024 * 1024),
    )(*pieces, inv_hi, inv_lo, rhs)


def shards(residual, counts, assembly, level_two, block_inverse):
    highest = lax.Precision.HIGHEST
    high = lax.Precision.HIGH
    rows = level_two.shape[1]
    half = rows // 2
    width = level_two.shape[2]
    block = block_inverse.shape[2]
    held = rows // block
    slots = assembly.shape[1]
    prim = assembly.shape[2]
    dofs = slots * prim
    nsub = lax.axis_size("sub")
    me = lax.axis_index("sub")

    def swap(value, dist):
        return lax.ppermute(value, "sub", [(i, i ^ dist) for i in range(nsub)])

    def weight(dist):
        return bin(dist).count("1")

    matrix = level_two[0]
    inv_own = block_inverse[0].reshape(held, block, block)
    paired = held % 2 == 0

    def own(value, c):
        return lax.dynamic_slice(value, (0, (me ^ c) * rows), (rows, rows))

    def plain(value):
        return with_layout_constraint(value, Layout(major_to_minor=tuple(range(value.ndim))))

    pairs = [(d, e) for d in range(1, nsub) for e in range(d + 1, nsub)]
    if paired:
        order = me
        span = -(-rows // LANE) * LANE
        early, moved, where = [], [], []
        for d, e in pairs:
            if weight(d) < weight(e):
                where.append(("block", d, e, d))
            elif weight(e) < weight(d):
                where.append(("turned", d, e, e))
        for kind, d, e, dist in where:
            early.append(plain(own(matrix, d ^ e)))
        early = list(lax.optimization_barrier(tuple(early)))
        for (kind, d, e, dist), value in zip(where, early):
            moved.append((swap(value, dist), kind, d, e))
        matrix, inv_own, residual, assembly, *early = lax.optimization_barrier(
            (matrix, inv_own, residual, assembly, *early)
        )
        inv_pack = pack_pairs(inv_own[: held // 2], inv_own[held // 2 :])
        arrived = [swap(inv_pack, d) for d in range(1, nsub)]
    else:
        order = 0
        span = rows
        full = lax.all_gather(matrix, "sub", axis=0, tiled=True)
        inverse = lax.all_gather(inv_own, "sub", axis=0, tiled=True)

    local = lax.all_to_all(residual, "owner", split_axis=1, concat_axis=0, tiled=True)
    cols = local.shape[0] // nsub
    flat = assembly[0].reshape(dofs, width)
    target = jnp.sum(flat * lax.broadcasted_iota(jnp.int32, (dofs, width), 1), axis=1)
    live = lax.broadcasted_iota(jnp.int32, (slots, prim), 1) < counts[0][:, None]
    target = jnp.where(live.reshape(dofs), target, -1).astype(jnp.float32)
    sends = []
    for d in range(nsub):
        piece = lax.dynamic_slice(local, ((me ^ d) * cols, 0), (cols, dofs))
        piece = jnp.concatenate([piece, target[None]], axis=0)
        sends.append(piece)
    if paired:
        here = own(matrix, 0)
        matrix, *sends = lax.optimization_barrier((matrix, *sends))
    columns = [value if d == 0 else swap(value, d) for d, value in enumerate(sends)]
    if paired:
        pieces, kinds = [], []

        def add(value, kind, d, e):
            pieces.append(value)
            kinds.append((kind, d, e))

        cut = half // LANE * LANE
        rest = rows - cut
        first = jnp.pad(here[:cut, :cut], ((0, rest - cut), (0, rest - cut)))
        mixed = pack_pairs(first, here[cut:, cut:])
        diag_pack = plain(
            jnp.concatenate(
                [here[cut:, :cut], mixed[:rest], jnp.transpose(mixed[rest:])], axis=1
            )
        )
        add(here, "block", 0, 0)
        for c in range(1, nsub):
            kept = [v for v, (_, d, e, _) in zip(early, where) if d ^ e == c]
            add(kept[0] if kept else plain(own(matrix, c)), "block", 0, c)
        for item in moved:
            add(*item)
        for d in range(1, nsub):
            add(plain(swap(diag_pack, d)), "diag", d, d)
        for d, e in pairs:
            if weight(d) == weight(e):
                both = own(matrix, d ^ e)
                upper, lower = plain(both[:half]), plain(jnp.transpose(both[:, half:]))
                upper, lower, diag_pack, *arrived = lax.optimization_barrier(
                    (upper, lower, diag_pack, *arrived)
                )
                add(plain(swap(upper, d)), "top", d, e)
                add(plain(swap(lower, e)), "bottom", d, e)
        inverses = [inv_own]
        for got in arrived:
            inverses.append(jnp.concatenate(unpack_pairs(got), axis=0))
        inverse = jnp.concatenate(inverses, axis=0).reshape(nsub, rows, block)
        wide = jnp.concatenate([inverse] * held, axis=2)
        row = lax.broadcasted_iota(jnp.int32, wide.shape, 1) // block
        col = lax.broadcasted_iota(jnp.int32, wide.shape, 2) // block
        wide = jnp.where(row == col, wide, 0.0)
        wide = jnp.pad(wide, ((0, 0), (0, span - rows), (0, span - rows))).reshape(nsub * span, span)
        top = lax.reduce_precision(wide, 8, 7)
        inv_hi, inv_lo = top.astype(jnp.bfloat16), (wide - top).astype(jnp.bfloat16)
    every = jnp.concatenate(columns, axis=1)
    mine = every[:cols]
    goal = every[cols].astype(jnp.int32)
    relative = jnp.where(goal < 0, -1, ((goal // rows) ^ order) * span + goal % rows)
    basis = (
        relative[:, None] == lax.broadcasted_iota(jnp.int32, (nsub * dofs, nsub * span), 1)
    ).astype(jnp.float32)
    resid = jnp.dot(mine, basis, precision=highest, preferred_element_type=jnp.float32)

    def precond(vector):
        shaped = vector.reshape(cols, width // block, block)
        return jnp.einsum("rbi,bij->rbj", shaped, inverse, precision=high).reshape(cols, width)

    def row_sum(left, right):
        return jnp.sum(left * right, axis=1, keepdims=True)

    if paired:
        answer, resid = solve(pieces, kinds, inv_hi, inv_lo, resid, nsub, rows, half, cut)
    else:
        answer = jnp.zeros_like(resid)
        zvec = precond(resid)
        direction = zvec
        rz_now = row_sum(resid, zvec)
        for step in range(ITERS):
            image = jnp.dot(direction, full, precision=high, preferred_element_type=jnp.float32)
            alpha = rz_now / row_sum(direction, image)
            answer = answer + alpha * direction
            resid = resid - alpha * image
            if step + 1 < ITERS:
                zvec = precond(resid)
                rz_next = row_sum(resid, zvec)
                direction = zvec + rz_next / rz_now * direction
                rz_now = rz_next
    corr = lax.dot_general(
        answer, basis, (((1,), (1,)), ((), ())), precision=high,
        preferred_element_type=jnp.float32,
    )

    def back(array, size, step, first):
        got = []
        for d in range(nsub):
            piece = lax.dynamic_slice(array, (0, (d ^ first) * step), (cols, size))
            got.append(piece if d == 0 else swap(piece, d))
        got = jnp.stack(got)
        return jnp.concatenate(
            [lax.dynamic_index_in_dim(got, me ^ c, 0, keepdims=False) for c in range(nsub)], axis=0
        )

    level_residual = back(resid, rows, span, 0 if paired else me)
    corrections = lax.all_to_all(
        back(corr, dofs, dofs, 0), "owner", split_axis=0, concat_axis=1, tiled=True
    )
    return (corrections, jnp.transpose(level_residual)[None])


def solution(mesh):
    in_specs = (
        P("owner", "sub"),
        P("owner", "sub"),
        P("owner", "sub", None, None),
        P("owner", "sub", None),
        P("owner", "sub", None),
    )
    out_specs = (P("owner", "sub"), P("owner", "sub", None))
    return jax.shard_map(shards, mesh=mesh, in_specs=in_specs, out_specs=out_specs, check_vma=False)
```
